32 devices in a mesh: groups: 2 (over x), rows: 16 (over z, y, core).
Axes of the slice: x: 2, y: 2, z: 4, core: 2. Of those that a mesh axis runs over, the one named last changes fastest.
Arguments:
- queries: bfloat16 [2048, 8192], P(('groups', 'rows')), parts along dimension 0, may hold values from -6 to 6
- sketches: bfloat16 [16384, 8192], P(('groups', 'rows')), parts along dimension 0, may hold values from -16 to 16, as said below
- row_ids: int32 [16384], P(('groups', 'rows')), parts along dimension 0, may hold values from 0 to 8191, each once
Outputs:
- top_scores: float32 [2048, 128], P(('groups', 'rows')), parts along dimension 0
The draws below stay inside these ranges and needn't reach their ends.
There are 2 independent parts, one for each index of `groups`. The reference program is written for one: setup_inputs(seed, part) draws one part's arguments, and reference() takes and returns one part's arrays. A program takes and returns all parts, laid end to end along the dimension named above; each array names one. Nothing has to cross between parts.
Inputs may be any that keep to these rules, and one draw needn't show every extreme that they name: `sketches`: sketch entries are real-valued.
All inputs are finite; a program needn't handle non-finite values.
Results may differ from the reference program's by a relative error of at most 0.0003.
Values may be sent and summed in bfloat16 or wider, within the bound.
A program may use at most 128 MiB of HBM per device.

```python
import jax
import jax.numpy as jnp
from jax import lax

WIDTH = 8192
NQ = 1024
ROWS_DEV = 512
TOPK = 128
ROWS = 8192
RETIRED = 2048
N_ROWS = 16


def query_values(key):
    values = jax.random.normal(jax.random.fold_in(key, 21), (NQ, WIDTH), jnp.float32)
    return jnp.clip(values, -6.0, 6.0)


def draw_queries(key, part):
    return query_values(key).astype(jnp.bfloat16)


def draw_sketches(key, part):
    position = jnp.arange(ROWS).astype(jnp.float32)
    rising = 1.0 + 2.0 * position / jnp.float32(max(ROWS - 1, 1))
    row_scale = jnp.exp(jax.random.uniform(jax.random.fold_in(key, 11), (ROWS,), jnp.float32, 0.0, jnp.log(10.0)))
    base = jax.random.normal(jax.random.fold_in(key, 14), (ROWS, WIDTH), jnp.float32)
    values = base * (row_scale * rising)[:, None] / jnp.sqrt(jnp.float32(WIDTH))
    query_full = query_values(key)
    home_query = jax.random.permutation(jax.random.fold_in(key, 31), NQ).astype(jnp.int32)[:N_ROWS]
    device_of_row = jnp.arange(ROWS).astype(jnp.int32) // ROWS_DEV
    scattered = jax.random.randint(jax.random.fold_in(key, 33), (ROWS,), 0, NQ).astype(jnp.int32)
    home_pool = jax.random.randint(jax.random.fold_in(key, 34), (ROWS,), 0, 2).astype(jnp.int32) == 0
    target = jnp.where(home_pool, jnp.take(home_query, device_of_row, axis=0), scattered).astype(jnp.int32)
    direction = jnp.take(query_full, target, axis=0) / jnp.float32(WIDTH)
    amplitude = 120.0 * jnp.exp(jax.random.uniform(jax.random.fold_in(key, 32), (ROWS,), jnp.float32, jnp.log(1.5), jnp.log(3.0)))
    boosted = values + amplitude[:, None] * direction
    return jnp.clip(boosted, -16.0, 16.0).astype(jnp.bfloat16)


def setup_inputs(seed: int = 0, part: int = 0) -> dict:
    streams_of = jax.random.split(jax.random.key(seed), 4)
    part_splits = jax.random.split(jax.random.fold_in(streams_of[3], part), 4)
    queries = draw_queries(jax.random.fold_in(jax.random.fold_in(streams_of[3], part), 71), part)
    sketches = draw_sketches(jax.random.fold_in(jax.random.fold_in(streams_of[3], part), 71), part)
    row_ids = jax.random.permutation(part_splits[2], ROWS).astype(jnp.int32)
    return {"queries": queries, "sketches": sketches, "row_ids": row_ids}


def reference(queries, sketches, row_ids):
    scores = lax.dot_general(queries, sketches, (((1,), (1,)), ((), ())), preferred_element_type=jnp.float32)
    live = row_ids >= RETIRED
    square_sum = lax.optimization_barrier(jnp.sum(jnp.where(live[None, :], scores * scores, jnp.float32(0.0)), axis=1))
    inverse_scale = lax.rsqrt(square_sum / jnp.float32(ROWS - RETIRED) + jnp.float32(1e-06))
    masked = jnp.where(live[None, :], scores, jnp.float32(-1e+30))
    best = lax.top_k(masked, TOPK)[0]
    return best * inverse_scale[:, None]
```

```python
import functools

import jax
import jax.numpy as jnp
from jax import lax
from jax.experimental import pallas as pl
from jax.experimental.pallas import tpu as pltpu
from jax.sharding import PartitionSpec as P

TOPK = 128
LANES = 128
SUBLANES = 8
SPLIT = 4
NEG = -1e30
MESH = pl.DeviceIdType.MESH


def exchange(x, low, high, dist):
    n = x.shape[0]
    mid = x[low:high].reshape((high - low) // (2 * dist), 2, dist, SUBLANES, LANES)
    a, b = mid[:, 0], mid[:, 1]
    mid = jnp.concatenate([jnp.maximum(a, b)[:, None], jnp.minimum(a, b)[:, None]], axis=1)
    mid = mid.reshape(high - low, SUBLANES, LANES)
    parts = ([x[:low]] if low else []) + [mid] + ([x[high:]] if high < n else [])
    return jnp.concatenate(parts, axis=0) if len(parts) > 1 else mid


def sort_rows(x):
    n = x.shape[0]
    p = 1
    while p < n:
        x = exchange(x, 0, n, p)
        k = p // 2
        while k >= 1:
            blocks = x.reshape(n // (2 * p), 2 * p, SUBLANES, LANES)
            mid = blocks[:, k : 2 * p - k]
            count = (2 * p - 2 * k) // (2 * k)
            mid = mid.reshape(n // (2 * p), count, 2, k, SUBLANES, LANES)
            a, b = mid[:, :, 0], mid[:, :, 1]
            mid = jnp.concatenate([jnp.maximum(a, b)[:, :, None], jnp.minimum(a, b)[:, :, None]], axis=2)
            mid = mid.reshape(n // (2 * p), 2 * p - 2 * k, SUBLANES, LANES)
            x = jnp.concatenate([blocks[:, :k], mid, blocks[:, 2 * p - k :]], axis=1).reshape(n, SUBLANES, LANES)
            k //= 2
        p *= 2
    return x


def reverse_rows(x):
    n = x.shape[0]
    d = n // 2
    while d >= 1:
        y = x.reshape(n // (2 * d), 2, d, SUBLANES, LANES)
        x = jnp.concatenate([y[:, 1:], y[:, :1]], axis=1).reshape(n, SUBLANES, LANES)
        d //= 2
    return x


def merge_rolled(x, shift, axis):
    n = x.shape[0]
    size = x.shape[axis]
    rolled = pltpu.roll(x, size - shift, axis)
    x = jnp.maximum(x, reverse_rows(rolled))
    d = n // 2
    while d >= 1:
        x = exchange(x, 0, n, d)
        d //= 2
    return x


def compact(x):
    n = x.shape[0]
    y = x.reshape(n // SUBLANES, SUBLANES, SUBLANES, LANES)
    sub = lax.broadcasted_iota(jnp.int32, (n // SUBLANES, SUBLANES, LANES), 1)
    out = y[:, 0]
    for s in range(1, SUBLANES):
        out = jnp.where(sub == s, y[:, s], out)
    return out.reshape(n, LANES)


def kernel(n, retired, live_count, q_in, sk_in, id_in, out, qb, sk, idb, acc, sendb, recvb, tb,
           q_send, q_recv, c_send, c_recv, s_load, s_send, s_recv, own_sem, id_sem):
    nq, width = q_in.shape
    rows = sk_in.shape[0]
    wk = width // SPLIT
    per = LANES // nq
    groups = n // per
    steps = per // 2
    last = n // 2 - 1
    device = lax.axis_index("rows")
    core = device % 2
    chip = device // 2
    pos = chip // 2 + (chip % 2) * (n - 1 - 2 * (chip // 2))

    def at(position):
        p = (position + n) % n
        h = p // (n // 2)
        c = (1 - h) * (2 * p) + h * (2 * (n - 1 - p) + 1)
        return {"rows": c * 2 + core}

    right, left = at(pos + 1), at(pos - 1)
    partner = {"rows": chip * 2 + 1 - core}
    own = n - 1

    def slot_rows(slot):
        return pl.ds(pl.multiple_of(slot * nq, nq), nq)

    loads = []
    for s in range(SPLIT):
        loads.append(pltpu.make_async_copy(q_in.at[:, pl.ds(s * wk, wk)], qb.at[s, slot_rows(own)], own_sem.at[s]))
    for copy in loads:
        copy.start()
    sk_loads = []
    for s in range(SPLIT):
        sk_loads.append(pltpu.make_async_copy(sk_in.at[:, pl.ds(s * wk, wk)], sk.at[s, pl.ds(0, rows)], s_load.at[s]))
    for copy in sk_loads:
        copy.start()

    barrier = pltpu.get_barrier_semaphore()
    for j in range(1, n):
        pl.semaphore_signal(barrier, inc=1, device_id=at(pos + j), device_id_type=MESH)
    pl.semaphore_signal(barrier, inc=1, device_id=partner, device_id_type=MESH)
    pl.semaphore_wait(barrier, n)

    def q_copy(s, src, dst, target):
        return pltpu.make_async_remote_copy(
            src_ref=qb.at[s, slot_rows(src)], dst_ref=qb.at[s, slot_rows(dst)],
            send_sem=q_send.at[s, dst], recv_sem=q_recv.at[s, dst],
            device_id=target, device_id_type=MESH)

    for s in range(SPLIT):
        loads[s].wait()
        q_copy(s, own, 0, right).start()
        q_copy(s, own, 1, left).start()
    sk_sends = []
    for s in range(SPLIT):
        sk_sends.append(pltpu.make_async_remote_copy(
            src_ref=sk_in.at[:, pl.ds(s * wk, wk)], dst_ref=sk.at[s, pl.ds(rows, rows)],
            send_sem=s_send.at[s], recv_sem=s_recv.at[s], device_id=partner, device_id_type=MESH))
    id_send = pltpu.make_async_remote_copy(
        src_ref=id_in, dst_ref=idb.at[pl.ds(rows, rows)], send_sem=id_sem.at[0], recv_sem=id_sem.at[1],
        device_id=partner, device_id_type=MESH)
    for copy in sk_sends:
        copy.start()
    id_send.start()
    idb[pl.ds(0, rows)] = id_in[...]
    for copy in sk_loads:
        copy.wait()
    for copy in sk_sends:
        copy.wait()
    id_send.wait()

    def arrive(t, s):
        q_copy(s, 2 * t - 2, 2 * t - 2, right).wait_recv()
        q_copy(s, 2 * t - 1, 2 * t - 1, left).wait_recv()

        @pl.when(t < last)
        def _():
            q_copy(s, 2 * t - 2, 2 * t, right).start()
            q_copy(s, 2 * t - 1, 2 * t + 1, left).start()

        @pl.when((t == last) & (s < SPLIT // 2))
        def _():
            q_copy(s, 2 * t - 2, n - 2, right).start()

        @pl.when((t == last) & (s >= SPLIT // 2))
        def _():
            q_copy(s, 2 * t - 1, n - 2, left).start()

    def multiply(g, s):
        q = qb[s, pl.ds(pl.multiple_of(g * LANES, LANES), LANES)]
        acc[...] += lax.dot_general(sk[s], q, (((1,), (1,)), ((), ())), preferred_element_type=jnp.float32)

    def c_copy(slot, target):
        return pltpu.make_async_remote_copy(
            src_ref=sendb.at[slot], dst_ref=recvb.at[slot],
            send_sem=c_send.at[slot], recv_sem=c_recv.at[slot], device_id=target, device_id_type=MESH)

    def select(g, store_own):
        live = idb[...] >= retired
        scores = acc[...]
        square = jnp.where(live, scores * scores, 0.0).reshape(2 * rows // SUBLANES, SUBLANES, LANES).sum(axis=0)
        x = jnp.where(live, scores, NEG).reshape(2 * rows // SUBLANES, SUBLANES, LANES)
        x = sort_rows(x)
        shift = SUBLANES // 2
        while shift >= 1:
            x = merge_rolled(x, shift, 1)
            shift //= 2
        y = compact(x).T
        for p in range(per):
            slot = g * per + p
            target = recvb if store_own and p == per - 1 else sendb
            target[slot, pl.ds(0, nq)] = y[p * nq : (p + 1) * nq]
            target[slot, pl.ds(nq, SUBLANES)] = square
        for p in range(per - 1 if store_own else per):
            slot = g * per + p
            t = slot // 2 + 1
            c_copy(slot, at(pos - t) if p % 2 == 0 else at(pos + t)).start()

    def group(g, carry):
        acc[...] = jnp.zeros_like(acc)

        @pl.loop(0, steps)
        def _(u):
            @pl.loop(0, SPLIT)
            def _(s):
                arrive(g * steps + u + 1, s)
                if steps == 1:
                    multiply(g, s)

        if steps > 1:
            @pl.loop(0, SPLIT)
            def _(s):
                multiply(g, s)

        select(g, False)
        return carry

    lax.fori_loop(0, groups - 1, group, 0)

    acc[...] = jnp.zeros_like(acc)
    if steps > 1:
        @pl.loop(0, steps - 1)
        def _(u):
            @pl.loop(0, SPLIT)
            def _(s):
                arrive((groups - 1) * steps + u + 1, s)

    @pl.loop(0, SPLIT // 2)
    def _(h):
        for s in (h, h + SPLIT // 2):
            q_copy(s, n - 2, n - 2, right).wait_recv()
            multiply(groups - 1, s)

    select(groups - 1, True)

    @pl.loop(0, n - 2)
    def _(slot):
        @pl.loop(0, SPLIT)
        def _(s):
            q_copy(s, slot, slot, right).wait_send()

    @pl.loop(0, SPLIT)
    def _(s):
        q_copy(s, n - 2, n - 2, right).wait_send()

    @pl.loop(0, n - 1)
    def _(slot):
        c_copy(slot, right).wait()

    square = jnp.zeros((SUBLANES, LANES), jnp.float32)
    for p in range(per):
        part = recvb[p, pl.ds(nq, SUBLANES)]
        for g in range(1, groups):
            part += recvb[g * per + p, pl.ds(nq, SUBLANES)]
        square += pltpu.roll(part, (LANES - p * nq) % LANES, 1) if p else part
    total = jnp.sum(square, axis=0, keepdims=True)
    scale = lax.rsqrt(total / jnp.float32(live_count) + jnp.float32(1e-06))

    for g in range(groups):
        y = jnp.concatenate([recvb[g * per + p, pl.ds(0, nq)] for p in range(per)], axis=0).T
        for copy in range(SUBLANES // groups):
            tb[pl.ds((copy * groups + g) * TOPK, TOPK)] = y
    x = jnp.concatenate([tb[pl.ds(i, SUBLANES, TOPK)][None] for i in range(TOPK)], axis=0)
    shift = groups // 2
    while shift >= 1:
        x = merge_rolled(x, shift, 1)
        shift //= 2
    shift = LANES // 2
    while shift >= nq:
        x = merge_rolled(x, shift, 2)
        shift //= 2
    out[...] = (compact(x) * scale).T[:nq]


def shards(queries, sketches, row_ids):
    devices = lax.axis_size("rows")
    total_rows = sketches.shape[0] * devices
    retired = total_rows // 4
    live_count = total_rows - retired
    n = devices // 2
    nq, width = queries.shape
    rows = sketches.shape[0]
    wk = width // SPLIT
    ids = jnp.broadcast_to(row_ids[:, None], (rows, LANES))
    vmem = pl.BlockSpec(memory_space=pltpu.VMEM)
    hbm = pl.BlockSpec(memory_space=pl.ANY)
    return pl.pallas_call(
        functools.partial(kernel, n, retired, live_count),
        out_shape=jax.ShapeDtypeStruct((nq, TOPK), jnp.float32),
        in_specs=[hbm, hbm, vmem],
        out_specs=vmem,
        scratch_shapes=[
            pltpu.VMEM((SPLIT, n * nq, wk), jnp.bfloat16),
            pltpu.VMEM((SPLIT, 2 * rows, wk), jnp.bfloat16),
            pltpu.VMEM((2 * rows, LANES), jnp.int32),
            pltpu.VMEM((2 * rows, LANES), jnp.float32),
            pltpu.VMEM((n, nq + SUBLANES, TOPK), jnp.float32),
            pltpu.VMEM((n, nq + SUBLANES, TOPK), jnp.float32),
            pltpu.VMEM((SUBLANES * TOPK, LANES), jnp.float32),
            pltpu.SemaphoreType.DMA((SPLIT, n)),
            pltpu.SemaphoreType.DMA((SPLIT, n)),
            pltpu.SemaphoreType.DMA((n,)),
            pltpu.SemaphoreType.DMA((n,)),
            pltpu.SemaphoreType.DMA((SPLIT,)),
            pltpu.SemaphoreType.DMA((SPLIT,)),
            pltpu.SemaphoreType.DMA((SPLIT,)),
            pltpu.SemaphoreType.DMA((SPLIT,)),
            pltpu.SemaphoreType.DMA((2,)),
        ],
        compiler_params=pltpu.CompilerParams(
            collective_id=0, has_side_effects=True, vmem_limit_bytes=60 * 1024 * 1024
        ),
        name="attribution",
    )(queries, sketches, ids)


def solution(mesh):
    return jax.shard_map(
        shards,
        mesh=mesh,
        in_specs=(P(("groups", "rows"), None), P(("groups", "rows"), None), P(("groups", "rows"))),
        out_specs=P(("groups", "rows"), None),
        check_vma=False,
    )
```

```python
import functools

import jax
import jax.numpy as jnp
from jax import lax
from jax.experimental import pallas as pl
from jax.experimental.pallas import tpu as pltpu
from jax.sharding import PartitionSpec as P

TOPK = 128
LANES = 128
SUBLANES = 8
SPLIT = 8
NEG = -1e30
MESH = pl.DeviceIdType.MESH


def exchange(x, low, high, dist):
    n = x.shape[0]
    mid = x[low:high].reshape((high - low) // (2 * dist), 2, dist, SUBLANES, LANES)
    a, b = mid[:, 0], mid[:, 1]
    mid = jnp.concatenate([jnp.maximum(a, b)[:, None], jnp.minimum(a, b)[:, None]], axis=1)
    mid = mid.reshape(high - low, SUBLANES, LANES)
    parts = ([x[:low]] if low else []) + [mid] + ([x[high:]] if high < n else [])
    return jnp.concatenate(parts, axis=0) if len(parts) > 1 else mid


def sort_rows(x):
    n = x.shape[0]
    p = 1
    while p < n:
        x = exchange(x, 0, n, p)
        k = p // 2
        while k >= 1:
            blocks = x.reshape(n // (2 * p), 2 * p, SUBLANES, LANES)
            mid = blocks[:, k : 2 * p - k]
            count = (2 * p - 2 * k) // (2 * k)
            mid = mid.reshape(n // (2 * p), count, 2, k, SUBLANES, LANES)
            a, b = mid[:, :, 0], mid[:, :, 1]
            mid = jnp.concatenate([jnp.maximum(a, b)[:, :, None], jnp.minimum(a, b)[:, :, None]], axis=2)
            mid = mid.reshape(n // (2 * p), 2 * p - 2 * k, SUBLANES, LANES)
            x = jnp.concatenate([blocks[:, :k], mid, blocks[:, 2 * p - k :]], axis=1).reshape(n, SUBLANES, LANES)
            k //= 2
        p *= 2
    return x


def reverse_rows(x):
    n = x.shape[0]
    d = n // 2
    while d >= 1:
        y = x.reshape(n // (2 * d), 2, d, SUBLANES, LANES)
        x = jnp.concatenate([y[:, 1:], y[:, :1]], axis=1).reshape(n, SUBLANES, LANES)
        d //= 2
    return x


def merge_rolled(x, shift, axis):
    n = x.shape[0]
    size = x.shape[axis]
    rolled = pltpu.roll(x, size - shift, axis)
    x = jnp.maximum(x, reverse_rows(rolled))
    d = n // 2
    while d >= 1:
        x = exchange(x, 0, n, d)
        d //= 2
    return x


def compact(x):
    n = x.shape[0]
    y = x.reshape(n // SUBLANES, SUBLANES, SUBLANES, LANES)
    sub = lax.broadcasted_iota(jnp.int32, (n // SUBLANES, SUBLANES, LANES), 1)
    out = y[:, 0]
    for s in range(1, SUBLANES):
        out = jnp.where(sub == s, y[:, s], out)
    return out.reshape(n, LANES)


def kernel(n, retired, live_count, q_in, sk_in, id_in, out, qb, sk, idb, acc, sendb, recvb, tb,
           q_send, q_recv, c_send, c_recv, s_load, s_send, s_recv, own_sem, id_sem, id_load_sem):
    nq, width = q_in.shape
    rows = sk_in.shape[0]
    wk = width // SPLIT
    per = LANES // nq
    groups = n // per
    steps = per // 2
    last = n // 2 - 1
    device = lax.axis_index("rows")
    core = device % 2
    chip = device // 2
    pos = chip // 2 + (chip % 2) * (n - 1 - 2 * (chip // 2))

    def at(position):
        p = (position + n) % n
        h = p // (n // 2)
        c = (1 - h) * (2 * p) + h * (2 * (n - 1 - p) + 1)
        return {"rows": c * 2 + core}

    right, left = at(pos + 1), at(pos - 1)
    partner = {"rows": chip * 2 + 1 - core}
    own = n - 1

    def slot_rows(slot):
        return pl.ds(pl.multiple_of(slot * nq, nq), nq)

    loads = []
    for s in range(SPLIT):
        loads.append(pltpu.make_async_copy(q_in.at[:, pl.ds(s * wk, wk)], qb.at[s, slot_rows(own)], own_sem.at[s]))
    for copy in loads:
        copy.start()
    sk_loads = []
    for s in range(SPLIT):
        sk_loads.append(pltpu.make_async_copy(sk_in.at[:, pl.ds(s * wk, wk)], sk.at[s, pl.ds(0, rows)], s_load.at[s]))
    for copy in sk_loads:
        copy.start()
    id_load = pltpu.make_async_copy(id_in, idb.at[pl.ds(0, rows)], id_load_sem.at[0])
    id_load.start()

    barrier = pltpu.get_barrier_semaphore()
    for j in range(1, n):
        pl.semaphore_signal(barrier, inc=1, device_id=at(pos + j), device_id_type=MESH)
    pl.semaphore_signal(barrier, inc=1, device_id=partner, device_id_type=MESH)
    pl.semaphore_wait(barrier, n)

    def q_copy(s, src, dst, target):
        return pltpu.make_async_remote_copy(
            src_ref=qb.at[s, slot_rows(src)], dst_ref=qb.at[s, slot_rows(dst)],
            send_sem=q_send.at[s, dst], recv_sem=q_recv.at[s, dst],
            device_id=target, device_id_type=MESH)

    for s in range(SPLIT):
        loads[s].wait()
        q_copy(s, own, 0, right).start()
        q_copy(s, own, 1, left).start()
    sk_sends = []
    for s in range(SPLIT):
        sk_sends.append(pltpu.make_async_remote_copy(
            src_ref=sk_in.at[:, pl.ds(s * wk, wk)], dst_ref=sk.at[s, pl.ds(rows, rows)],
            send_sem=s_send.at[s], recv_sem=s_recv.at[s], device_id=partner, device_id_type=MESH))
    id_send = pltpu.make_async_remote_copy(
        src_ref=id_in, dst_ref=idb.at[pl.ds(rows, rows)], send_sem=id_sem.at[0], recv_sem=id_sem.at[1],
        device_id=partner, device_id_type=MESH)
    for copy in sk_sends:
        copy.start()
    id_send.start()
    id_load.wait()
    for copy in sk_loads:
        copy.wait()
    for copy in sk_sends:
        copy.wait()
    id_send.wait()

    def arrive(t, s):
        q_copy(s, 2 * t - 2, 2 * t - 2, right).wait_recv()
        q_copy(s, 2 * t - 1, 2 * t - 1, left).wait_recv()

        @pl.when(t < last)
        def _():
            q_copy(s, 2 * t - 2, 2 * t, right).start()
            q_copy(s, 2 * t - 1, 2 * t + 1, left).start()

        @pl.when((t == last) & (s < SPLIT // 2))
        def _():
            q_copy(s, 2 * t - 2, n - 2, right).start()

        @pl.when((t == last) & (s >= SPLIT // 2))
        def _():
            q_copy(s, 2 * t - 1, n - 2, left).start()

    def multiply(g, s):
        q = qb[s, pl.ds(pl.multiple_of(g * LANES, LANES), LANES)]
        acc[...] += lax.dot_general(sk[s], q, (((1,), (1,)), ((), ())), preferred_element_type=jnp.float32)

    def c_copy(slot, target):
        return pltpu.make_async_remote_copy(
            src_ref=sendb.at[slot], dst_ref=recvb.at[slot],
            send_sem=c_send.at[slot], recv_sem=c_recv.at[slot], device_id=target, device_id_type=MESH)

    def select(g, store_own):
        live = idb[...] >= retired
        scores = acc[...]
        square = jnp.where(live, scores * scores, 0.0).reshape(2 * rows // SUBLANES, SUBLANES, LANES).sum(axis=0)
        x = jnp.where(live, scores, NEG).reshape(2 * rows // SUBLANES, SUBLANES, LANES)
        x = sort_rows(x)
        shift = SUBLANES // 2
        while shift >= 1:
            x = merge_rolled(x, shift, 1)
            shift //= 2
        y = compact(x).T
        for p in range(per):
            slot = g * per + p
            target = recvb if store_own and p == per - 1 else sendb
            target[slot, pl.ds(0, nq)] = y[p * nq : (p + 1) * nq]
            target[slot, pl.ds(nq, SUBLANES)] = square
        for p in range(per - 1 if store_own else per):
            slot = g * per + p
            t = slot // 2 + 1
            c_copy(slot, at(pos - t) if p % 2 == 0 else at(pos + t)).start()

    def group(g, carry):
        acc[...] = jnp.zeros_like(acc)

        @pl.loop(0, steps)
        def _(u):
            @pl.loop(0, SPLIT)
            def _(s):
                arrive(g * steps + u + 1, s)
                if steps == 1:
                    multiply(g, s)

        if steps > 1:
            @pl.loop(0, SPLIT)
            def _(s):
                multiply(g, s)

        select(g, False)
        return carry

    lax.fori_loop(0, groups - 1, group, 0)

    acc[...] = jnp.zeros_like(acc)
    if steps > 1:
        @pl.loop(0, steps - 1)
        def _(u):
            @pl.loop(0, SPLIT)
            def _(s):
                arrive((groups - 1) * steps + u + 1, s)

    @pl.loop(0, SPLIT // 2)
    def _(h):
        for s in (h, h + SPLIT // 2):
            q_copy(s, n - 2, n - 2, right).wait_recv()
            multiply(groups - 1, s)

    select(groups - 1, True)

    @pl.loop(0, n - 2)
    def _(slot):
        @pl.loop(0, SPLIT)
        def _(s):
            q_copy(s, slot, slot, right).wait_send()

    @pl.loop(0, SPLIT)
    def _(s):
        q_copy(s, n - 2, n - 2, right).wait_send()

    @pl.loop(0, n - 2)
    def _(slot):
        c_copy(slot, right).wait()

    for g in range(groups):
        parts = [recvb[g * per + p, pl.ds(0, nq)] for p in range(per)]
        if g == groups - 1:
            parts[per - 2] = jnp.full((nq, TOPK), NEG, jnp.float32)
        y = jnp.concatenate(parts, axis=0).T
        for copy in range(SUBLANES // groups):
            tb[pl.ds((copy * groups + g) * TOPK, TOPK)] = y
    x = jnp.concatenate([tb[pl.ds(i, SUBLANES, TOPK)][None] for i in range(TOPK)], axis=0)
    shift = groups // 2
    while shift >= 1:
        x = merge_rolled(x, shift, 1)
        shift //= 2
    shift = LANES // 2
    while shift >= nq:
        x = merge_rolled(x, shift, 2)
        shift //= 2
    tb[pl.ds(0, TOPK)] = compact(reverse_rows(x))

    c_copy(n - 2, right).wait()
    square = jnp.zeros((SUBLANES, LANES), jnp.float32)
    for p in range(per):
        part = recvb[p, pl.ds(nq, SUBLANES)]
        for g in range(1, groups):
            part += recvb[g * per + p, pl.ds(nq, SUBLANES)]
        square += pltpu.roll(part, (LANES - p * nq) % LANES, 1) if p else part
    total = jnp.sum(square, axis=0, keepdims=True)
    scale = lax.rsqrt(total / jnp.float32(live_count) + jnp.float32(1e-06))

    late = recvb[n - 2, pl.ds(0, nq)]
    if nq < LANES:
        late = jnp.concatenate([late, jnp.zeros((LANES - nq, TOPK), jnp.float32)], axis=0)
    m = jnp.maximum(tb[pl.ds(0, TOPK)], late.T).reshape(TOPK // SUBLANES, SUBLANES, LANES)
    d = TOPK // SUBLANES // 2
    while d >= 1:
        m = exchange(m, 0, TOPK // SUBLANES, d)
        d //= 2
    sub = lax.broadcasted_iota(jnp.int32, m.shape, 1)
    d = SUBLANES // 2
    while d >= 1:
        after, before = pltpu.roll(m, SUBLANES - d, 1), pltpu.roll(m, d, 1)
        m = jnp.where((sub & d) == 0, jnp.maximum(m, after), jnp.minimum(m, before))
        d //= 2
    out[...] = (m.reshape(TOPK, LANES) * scale).T[:nq]


def shards(queries, sketches, row_ids):
    devices = lax.axis_size("rows")
    total_rows = sketches.shape[0] * devices
    retired = total_rows // 4
    live_count = total_rows - retired
    n = devices // 2
    nq, width = queries.shape
    rows = sketches.shape[0]
    wk = width // SPLIT
    ids = jnp.broadcast_to(row_ids[:, None], (rows, LANES))
    vmem = pl.BlockSpec(memory_space=pltpu.VMEM)
    hbm = pl.BlockSpec(memory_space=pl.ANY)
    return pl.pallas_call(
        functools.partial(kernel, n, retired, live_count),
        out_shape=jax.ShapeDtypeStruct((nq, TOPK), jnp.float32),
        in_specs=[hbm, hbm, hbm],
        out_specs=vmem,
        scratch_shapes=[
            pltpu.VMEM((SPLIT, n * nq, wk), jnp.bfloat16),
            pltpu.VMEM((SPLIT, 2 * rows, wk), jnp.bfloat16),
            pltpu.VMEM((2 * rows, LANES), jnp.int32),
            pltpu.VMEM((2 * rows, LANES), jnp.float32),
            pltpu.VMEM((n, nq + SUBLANES, TOPK), jnp.float32),
            pltpu.VMEM((n, nq + SUBLANES, TOPK), jnp.float32),
            pltpu.VMEM((SUBLANES * TOPK, LANES), jnp.float32),
            pltpu.SemaphoreType.DMA((SPLIT, n)),
            pltpu.SemaphoreType.DMA((SPLIT, n)),
            pltpu.SemaphoreType.DMA((n,)),
            pltpu.SemaphoreType.DMA((n,)),
            pltpu.SemaphoreType.DMA((SPLIT,)),
            pltpu.SemaphoreType.DMA((SPLIT,)),
            pltpu.SemaphoreType.DMA((SPLIT,)),
            pltpu.SemaphoreType.DMA((SPLIT,)),
            pltpu.SemaphoreType.DMA((2,)),
            pltpu.SemaphoreType.DMA((1,)),
        ],
        compiler_params=pltpu.CompilerParams(
            collective_id=0, has_side_effects=True, vmem_limit_bytes=60 * 1024 * 1024
        ),
        name="attribution",
    )(queries, sketches, ids)


def solution(mesh):
    return jax.shard_map(
        shards,
        mesh=mesh,
        in_specs=(P(("groups", "rows"), None), P(("groups", "rows"), None), P(("groups", "rows"))),
        out_specs=P(("groups", "rows"), None),
        check_vma=False,
    )
```
